32 devices in a mesh: gx: 4 (over z), gy: 2 (over y), gz: 4 (over x, core).
Axes of the slice: x: 2, y: 2, z: 4, core: 2. Of those that a mesh axis runs over, the one named last changes fastest.
Arguments:
- cell_volume: float32 [64, 32, 512], P('gx', 'gy', 'gz'), may hold values from 0.5 to 2
- exponent: int32 [64, 32, 512], P('gx', 'gy', 'gz'), may hold values from 0 to 7
- owner_row: int32 [8192], P(('gx', 'gy', 'gz')), may hold values from 0 to 8191, as said below
Outputs:
- stencil_out: float32 [27, 8192, 128], P(None, ('gx', 'gy', 'gz'))
- lumped_out: float32 [8192, 128], P(('gx', 'gy', 'gz'))
The draws below stay inside these ranges and needn't reach their ends.
Inputs may be any that keep to these rules, and one draw needn't show every extreme that they name: owner_row is a permutation of the row blocks; the row blocks of each device's share of owner_row go to each owner (owner_row // 256) exactly 8 times.
All inputs are finite; a program needn't handle non-finite values.
Results may differ from the reference program's by a relative error of at most 0.00007.
Values sent between devices are 32-bit elements; how exact they have to be, the bound alone decides.
A program may use at most 64 MiB of HBM per device.

```python
import math
import jax
import jax.numpy as jnp

EX = 16
EY = 16
EZ = 128
NX = 64
NY = 32
NZ = 512
LINES_DEV = 256
LINES = 8192
SENDS = 8
N_GX = 4
N_GY = 2
N_GZ = 4
DEVICES = 32


def draw_owner_row(key, part):
    source_keys = jax.random.split(jax.random.fold_in(key, 101), DEVICES)
    target_keys = jax.random.split(jax.random.fold_in(key, 202), DEVICES)
    source_perm = jax.vmap(lambda subkey: jax.random.permutation(subkey, LINES_DEV))(source_keys)
    target_perm = jax.vmap(lambda subkey: jax.random.permutation(subkey, LINES_DEV))(target_keys)
    owner_dev = source_perm % DEVICES
    rank_ids = source_perm // DEVICES
    source_ids = jnp.arange(DEVICES, dtype=jnp.int32)[:, None]
    slot_ids = target_perm[owner_dev, source_ids * SENDS + rank_ids]
    return (owner_dev * LINES_DEV + slot_ids).reshape(-1).astype(jnp.int32)


def with_ends(drawn, key, least, high):
    longest = drawn.shape.index(max(drawn.shape))
    spots = []
    for shift in (0, 1):
        where = [jax.random.randint(jax.random.fold_in(key, axis), (), 0, length) for axis, length in enumerate(drawn.shape)]
        where[longest] = (where[longest] + shift) % drawn.shape[longest]
        spots.append(tuple(where))
    return drawn.at[spots[0]].set(least).at[spots[1]].set(high)


def shard_levels(own_key, shape, cuts, low, top_value):
    level, own = 1.0, jax.random.fold_in(own_key, 6)
    for dim, shards_of in cuts:
        draws = jnp.exp(jax.random.uniform(jax.random.fold_in(own, dim), (shards_of,), jnp.float32, low / len(cuts), top_value / len(cuts)))
        level = level * jnp.repeat(draws, shape[dim] // shards_of).reshape([-1 if axis == dim else 1 for axis in range(len(shape))])
    return level


def setup_inputs(seed: int = 0) -> dict:
    key_of = jax.random.split(jax.random.key(seed), 4)
    return {
        "cell_volume": jnp.clip(jnp.exp(math.log(2.0) - 1.3862944 * jax.random.uniform(key_of[0], (NX, NY, NZ), jnp.float32) ** shard_levels(key_of[0], (NX, NY, NZ), ((0, 4), (1, 2), (2, 4)), -0.2, 0.2)), 0.5, 2.0),
        "exponent": with_ends(jax.random.randint(key_of[1], (NX, NY, NZ), 0, 8), jax.random.fold_in(key_of[1], 1), 0, 7).astype(jnp.int32),
        "owner_row": draw_owner_row(jax.random.fold_in(key_of[3], 71), 0),
    }


log_step = 0.3


def reference(cell_volume, exponent, owner_row):
    weight = cell_volume * jnp.exp(-log_step * exponent.astype(jnp.float32))
    current = weight[None, None, None]
    for along in range(3):
        behind = jnp.roll(current, 1, axis=3 + along)
        current = jnp.concatenate([behind, 2.0 * (current + behind), current], axis=along)
    stencil = current.reshape(27, NX, NY, NZ) * 0.015625
    lumped = 1.0 / jnp.sum(stencil, axis=0)
    stencil_lines = stencil.reshape(27, N_GX, EX, N_GY, EY, N_GZ, EZ).transpose(0, 1, 3, 5, 2, 4, 6).reshape(27, LINES, EZ)
    lumped_lines = lumped.reshape(N_GX, EX, N_GY, EY, N_GZ, EZ).transpose(0, 2, 4, 1, 3, 5).reshape(LINES, EZ)
    stencil_out = jnp.zeros((27, LINES, EZ), jnp.float32).at[:, owner_row].set(stencil_lines)
    lumped_out = jnp.zeros((LINES, EZ), jnp.float32).at[owner_row].set(lumped_lines)
    return (stencil_out, lumped_out)
```

```python
import functools

import jax
import jax.numpy as jnp
from jax import lax
from jax.experimental import pallas as pl
from jax.experimental.pallas import tpu as pltpu
from jax.sharding import PartitionSpec as P

MESH = pl.DeviceIdType.MESH
AXES = ("gx", "gy", "gz")
F32, BF16, I32 = jnp.float32, jnp.bfloat16, jnp.int32
log_step = 0.3
NN = (((1,), (0,)), ((), ()))
NT = (((1,), (1,)), ((), ()))


def onehot(mask):
    return jnp.where(mask, 1.0, 0.0).astype(BF16)


def split3(x):
    hi = x.astype(BF16)
    rest = x - hi.astype(F32)
    mid = rest.astype(BF16)
    return hi, mid, (rest - mid.astype(F32)).astype(BF16)


def pick(sel, x, dims=NN):
    total = None
    for part in split3(x):
        term = lax.dot_general(sel, part, dims, preferred_element_type=F32)
        total = term if total is None else total + term
    return total


def pick_r(x, sel, dims=NN):
    total = None
    for part in split3(x):
        term = lax.dot_general(part, sel, dims, preferred_element_type=F32)
        total = term if total is None else total + term
    return total


def iota(shape, dim):
    return lax.broadcasted_iota(I32, shape, dim)


def roll_lanes(x, shift):
    width = x.shape[1]
    cut = width - shift % width
    return jnp.concatenate([x[:, cut:], x[:, :cut]], axis=1)


def exchange(
    sizes, cv_ref, ex_ref, own_ref, cur_ref, bef_ref,
    sb1, sb2, rb1, rb2, tx, ty, tc, tr, hx, hy, hc, hr,
    s1_sem, s2_sem, r1_sem, r2_sem, hs_sem, hr_sem,
):
    nx, ny, nz = sizes
    n = nx * ny * nz
    gx, gy, gz = (lax.axis_index(a) for a in AXES)
    me = (gx * ny + gy) * nz + gz
    sx, sy, width = cv_ref.shape
    lines = sx * sy
    s = lines // n

    def coords(d):
        return (d // (ny * nz), (d // nz) % ny, d % nz)

    barrier = pltpu.get_barrier_semaphore()

    def greet(k, carry):
        d = (me + k) % n
        pl.semaphore_signal(barrier, inc=1, device_id=coords(d), device_id_type=MESH)
        return carry

    lax.fori_loop(1, n, greet, 0)

    w3 = cv_ref[...] * jnp.exp(-log_step * ex_ref[...].astype(F32))
    w = w3.reshape(lines, width)
    tx[...] = w[lines - sy :, :]
    ty[...] = w3[:, sy - 1 :, :]
    tc[...] = w[lines - 1 :, :]
    last = onehot(iota((8, width), 1) == width - 1)
    tr[...] = pick(last, w, NT)[0:1, :]

    owner_full = own_ref[...]
    owner = owner_full // lines
    slot = (owner_full % lines).astype(F32)
    mine = owner == iota((n, lines), 0)
    mine_b = onehot(mine)
    below = onehot(iota((lines, lines), 0) < iota((lines, lines), 1))
    counts = lax.dot_general(mine_b, below, NN, preferred_element_type=F32)
    rank = jnp.sum(jnp.where(mine, counts, 0.0), axis=0, keepdims=True).astype(I32)
    place = onehot(owner * s + rank == iota((lines, lines), 0))

    row_id = iota((width, lines), 0)
    at_rank = rank == row_id % s
    group = row_id // s

    packed0 = pick(place, w)
    sb1[:, 0:s, :] = packed0.reshape(n, s, width)
    slots = pick(mine_b, jnp.where(at_rank & (group == 0), slot, 0.0), NT)
    sb1[:, s : s + 1, :] = slots.reshape(n, 1, width)

    pl.semaphore_wait(barrier, n - 1)

    ux, uy, uz = (gx + 1) % nx, (gy + 1) % ny, (gz + 1) % nz
    halo = []
    routes = [
        (tx, hx, (ux, gy, gz)),
        (ty, hy, (gx, uy, gz)),
        (tc, hc, (ux, uy, gz)),
        (tr, hr.at[0], (gx, gy, uz)),
        (tr, hr.at[1], (ux, gy, uz)),
        (tr, hr.at[2], (gx, uy, uz)),
        (tr, hr.at[3], (ux, uy, uz)),
    ]
    for i, (src, dst, to) in enumerate(routes):
        copy = pltpu.make_async_remote_copy(
            src_ref=src, dst_ref=dst, send_sem=hs_sem.at[i], recv_sem=hr_sem.at[i],
            device_id=to, device_id_type=MESH,
        )
        copy.start()
        halo.append(copy)

    def send_all(sb, rb, s_sem, r_sem):
        def send(k, carry):
            d = (me + k) % n
            pltpu.make_async_remote_copy(
                src_ref=sb.at[d], dst_ref=rb.at[me], send_sem=s_sem, recv_sem=r_sem,
                device_id=coords(d), device_id_type=MESH,
            ).start()
            return carry

        lax.fori_loop(n // 2, n, send, 0)
        lax.fori_loop(1, n // 2, send, 0)
        pltpu.make_async_copy(sb.at[me], rb.at[me], r_sem).start()

    send_all(sb1, rb1, s1_sem, r1_sem)

    for copy in halo:
        copy.wait()

    line_id = iota((lines, width), 0)
    first_j = line_id % sy == 0

    def back_j(x, edge):
        edge_full = jnp.broadcast_to(edge, (sx, sy, width)).reshape(lines, width)
        shifted = jnp.concatenate([x[lines - 1 :, :], x[: lines - 1, :]], axis=0)
        return jnp.where(first_j, edge_full, shifted)

    x1 = jnp.concatenate([hx[...], w[: lines - sy, :]], axis=0)
    edge = hy[...]
    x2 = back_j(w, edge)
    x3 = back_j(x1, jnp.concatenate([hc[...].reshape(1, 1, width), edge[: sx - 1]], axis=0))
    for c, x in enumerate((x1, x2, x3)):
        sb2[:, c * s : (c + 1) * s, :] = pick(place, x).reshape(n, s, width)

    lane = iota((1, lines), 1)
    at_j0 = lane % sy == 0
    r0, rx, ry, rxy = hr[0], hr[1], hr[2], hr[3]
    rim1 = jnp.where(lane < sy, roll_lanes(rx, sy), roll_lanes(r0, sy))
    rim2 = jnp.where(at_j0, roll_lanes(ry, 1 - sy), roll_lanes(r0, 1))
    edge_rim = jnp.where(lane == 0, roll_lanes(rxy, 1), roll_lanes(ry, 1))
    rim3 = jnp.where(at_j0, edge_rim, roll_lanes(rim1, 1))
    rims = jnp.where(group == 0, r0, jnp.where(group == 1, rim1, jnp.where(group == 2, rim2, rim3)))
    rims = jnp.where(at_rank & (group < 4), rims, 0.0)
    sb2[:, 3 * s : 3 * s + 1, :] = pick(mine_b, rims, NT).reshape(n, 1, width)

    send_all(sb2, rb2, s2_sem, r2_sem)

    pltpu.make_async_copy(rb1, rb1, r1_sem).wait()
    col_id = iota((width, lines), 1)
    from_dev = iota((n, lines), 1) // s == iota((n, lines), 0)

    def spread(extra, q):
        sel = onehot(row_id == q * s + col_id % s)
        return jnp.sum(jnp.where(from_dev, pick_r(extra, sel), 0.0), axis=0, keepdims=True)

    slot_in = spread(rb1[:, s : s + 1, :].reshape(n, width), 0).astype(I32)
    to_slot = onehot(slot_in == iota((lines, lines), 0))
    cur_ref[0] = pick(to_slot, rb1[:, 0:s, :].reshape(lines, width))

    pltpu.make_async_copy(rb2, rb2, r2_sem).wait()
    for c in range(3):
        cur_ref[c + 1] = pick(to_slot, rb2[:, c * s : (c + 1) * s, :].reshape(lines, width))
    extra = rb2[:, 3 * s : 3 * s + 1, :].reshape(n, width)
    got = [spread(extra, q) for q in range(4)]
    rows = jnp.zeros((width, lines), F32)
    for q in range(4):
        rows = jnp.where(row_id == q, got[q], rows)
    bef_ref[...] = pick(to_slot, rows, NT)

    pltpu.make_async_copy(sb1.at[pl.ds(0, n - 1)], sb1.at[pl.ds(0, n - 1)], s1_sem).wait()
    pltpu.make_async_copy(sb2.at[pl.ds(0, n - 1)], sb2.at[pl.ds(0, n - 1)], s2_sem).wait()


def finish(cur_ref, bef_ref, out_ref, lump_ref):
    shape = cur_ref.shape[1:]
    at_0 = iota(shape, 1) == 0
    near, far = [], []
    for c in range(4):
        x = cur_ref[c] * 0.015625
        shifted = pltpu.roll(x, 1, axis=1)
        near.append(x)
        far.append(jnp.where(at_0, bef_ref[:, c : c + 1] * 0.015625, shifted))

    def triple(c, b):
        return (b, 2.0 * (c + b), c)

    def nine(v):
        by_x0 = triple(v[0], v[1])
        by_x1 = triple(v[2], v[3])
        return [triple(by_x0[o1], by_x1[o1]) for o1 in range(3)]

    cur, back = nine(near), nine(far)
    for o1 in range(3):
        for o2 in range(3):
            for o3, value in enumerate(triple(cur[o1][o2], back[o1][o2])):
                out_ref[9 * o1 + 3 * o2 + o3] = value
    total = functools.reduce(lambda a, b: a + b, near + far)
    lump_ref[...] = 1.0 / (27.0 * total)


def shards(sizes, cell_volume, exponent, owner_row):
    sx, sy, width = cell_volume.shape
    lines = sx * sy
    n = sizes[0] * sizes[1] * sizes[2]
    s = lines // n
    vmem = pl.BlockSpec(memory_space=pltpu.VMEM)
    dma = pltpu.SemaphoreType.DMA
    cur, bef = pl.pallas_call(
        functools.partial(exchange, sizes),
        out_shape=(
            jax.ShapeDtypeStruct((4, lines, width), F32),
            jax.ShapeDtypeStruct((lines, width), F32),
        ),
        in_specs=[vmem] * 3,
        out_specs=(vmem, vmem),
        scratch_shapes=[
            pltpu.VMEM((n, s + 1, width), F32),
            pltpu.VMEM((n, 3 * s + 1, width), F32),
            pltpu.VMEM((n, s + 1, width), F32),
            pltpu.VMEM((n, 3 * s + 1, width), F32),
            pltpu.VMEM((sy, width), F32),
            pltpu.VMEM((sx, 1, width), F32),
            pltpu.VMEM((1, width), F32),
            pltpu.VMEM((1, lines), F32),
            pltpu.VMEM((sy, width), F32),
            pltpu.VMEM((sx, 1, width), F32),
            pltpu.VMEM((1, width), F32),
            pltpu.VMEM((4, 1, lines), F32),
            dma, dma, dma, dma,
            dma((7,)),
            dma((7,)),
        ],
        compiler_params=pltpu.CompilerParams(collective_id=0, has_side_effects=True),
    )(cell_volume, exponent, owner_row.reshape(1, lines))
    rows = 64
    return pl.pallas_call(
        finish,
        grid=(lines // rows,),
        out_shape=(
            jax.ShapeDtypeStruct((27, lines, width), F32),
            jax.ShapeDtypeStruct((lines, width), F32),
        ),
        in_specs=[
            pl.BlockSpec((4, rows, width), lambda i: (0, i, 0)),
            pl.BlockSpec((rows, width), lambda i: (i, 0)),
        ],
        out_specs=(
            pl.BlockSpec((27, rows, width), lambda i: (0, i, 0)),
            pl.BlockSpec((rows, width), lambda i: (i, 0)),
        ),
    )(cur, bef)


def solution(mesh):
    sizes = tuple(mesh.shape[a] for a in AXES)
    return jax.shard_map(
        functools.partial(shards, sizes),
        mesh=mesh,
        in_specs=(P(*AXES), P(*AXES), P(AXES)),
        out_specs=(P(None, AXES, None), P(AXES, None)),
        check_vma=False,
    )
```

```python
import functools

import jax
import jax.numpy as jnp
from jax import lax
from jax.experimental import pallas as pl
from jax.experimental.pallas import tpu as pltpu
from jax.sharding import PartitionSpec as P

MESH = pl.DeviceIdType.MESH
AXES = ("gx", "gy", "gz")
F32, BF16, I32 = jnp.float32, jnp.bfloat16, jnp.int32
log_step = 0.3
NN = (((1,), (0,)), ((), ()))
NT = (((1,), (1,)), ((), ()))


def onehot(mask):
    return jnp.where(mask, 1.0, 0.0).astype(BF16)


def split3(x):
    hi = x.astype(BF16)
    rest = x - hi.astype(F32)
    mid = rest.astype(BF16)
    return hi, mid, (rest - mid.astype(F32)).astype(BF16)


def pick(sel, x, dims=NN):
    total = None
    for part in split3(x):
        term = lax.dot_general(sel, part, dims, preferred_element_type=F32)
        total = term if total is None else total + term
    return total


def pick_r(x, sel, dims=NN):
    total = None
    for part in split3(x):
        term = lax.dot_general(part, sel, dims, preferred_element_type=F32)
        total = term if total is None else total + term
    return total


def iota(shape, dim):
    return lax.broadcasted_iota(I32, shape, dim)


def roll_lanes(x, shift):
    width = x.shape[1]
    cut = width - shift % width
    return jnp.concatenate([x[:, cut:], x[:, :cut]], axis=1)


def exchange(
    sizes, cv_hbm, ex_hbm, own_hbm, cur_ref, bef_ref,
    cv_ref, ex_ref, own_ref, in_sem,
    sb1, sb2, sb3, rb1, rb2, rb3, tx, ty, tc, tr, hx, hy, hc, hr,
    s_sem, r_sem, hs_sem, hr_sem,
):
    nx, ny, nz = sizes
    n = nx * ny * nz
    gx, gy, gz = (lax.axis_index(a) for a in AXES)
    me = (gx * ny + gy) * nz + gz
    sx, sy, width = cv_ref.shape
    lines = sx * sy
    s = lines // n

    def coords(d):
        return (d // (ny * nz), (d // nz) % ny, d % nz)

    arrive = []
    for i, (src, dst) in enumerate(((own_hbm, own_ref), (cv_hbm, cv_ref), (ex_hbm, ex_ref))):
        copy = pltpu.make_async_copy(src, dst, in_sem.at[i])
        copy.start()
        arrive.append(copy)
    barrier = pltpu.get_barrier_semaphore()

    def greet(k, carry):
        d = (me + k) % n
        pl.semaphore_signal(barrier, inc=1, device_id=coords(d), device_id_type=MESH)
        return carry

    lax.fori_loop(1, n, greet, 0)

    arrive[0].wait()
    owner_full = own_ref[...]
    owner = owner_full // lines
    slot = (owner_full % lines).astype(F32)
    mine = owner == iota((n, lines), 0)
    mine_b = onehot(mine)
    below = onehot(iota((lines, lines), 0) < iota((lines, lines), 1))
    counts = lax.dot_general(mine_b, below, NN, preferred_element_type=F32)
    rank = jnp.sum(jnp.where(mine, counts, 0.0), axis=0, keepdims=True).astype(I32)
    place = onehot(owner * s + rank == iota((lines, lines), 0))

    row_id = iota((width, lines), 0)
    at_rank = rank == row_id % s
    group = row_id // s

    arrive[1].wait()
    arrive[2].wait()
    w3 = cv_ref[...] * jnp.exp(-log_step * ex_ref[...].astype(F32))
    w = w3.reshape(lines, width)
    tx[...] = w[lines - sy :, :]
    ty[...] = w3[:, sy - 1 :, :]
    tc[...] = w[lines - 1 :, :]
    last = onehot(iota((8, width), 1) == width - 1)
    tr[...] = pick(last, w, NT)[0:1, :]

    packed0 = pick(place, w)
    sb1[:, 0:s, :] = packed0.reshape(n, s, width)
    slots = pick(mine_b, jnp.where(at_rank & (group == 0), slot, 0.0), NT)
    sb1[:, s : s + 1, :] = slots.reshape(n, 1, width)

    pl.semaphore_wait(barrier, n - 1)

    ux, uy, uz = (gx + 1) % nx, (gy + 1) % ny, (gz + 1) % nz
    halo = []
    routes = [
        (ty, hy, (gx, uy, gz)),
        (tx, hx, (ux, gy, gz)),
        (tc, hc, (ux, uy, gz)),
        (tr, hr.at[0], (gx, gy, uz)),
        (tr, hr.at[1], (ux, gy, uz)),
        (tr, hr.at[2], (gx, uy, uz)),
        (tr, hr.at[3], (ux, uy, uz)),
    ]
    for i, (src, dst, to) in enumerate(routes):
        copy = pltpu.make_async_remote_copy(
            src_ref=src, dst_ref=dst, send_sem=hs_sem.at[i], recv_sem=hr_sem.at[i],
            device_id=to, device_id_type=MESH,
        )
        copy.start()
        halo.append(copy)

    def send_all(stage, sb, rb):
        def send(k, carry):
            d = (me + k) % n
            pltpu.make_async_remote_copy(
                src_ref=sb.at[d], dst_ref=rb.at[me], send_sem=s_sem.at[stage], recv_sem=r_sem.at[stage],
                device_id=coords(d), device_id_type=MESH,
            ).start()
            return carry

        lax.fori_loop(n // 2, n, send, 0)
        lax.fori_loop(ny * nz, n // 2, send, 0)
        lax.fori_loop(1, ny * nz, send, 0)
        pltpu.make_async_copy(sb.at[me], rb.at[me], r_sem.at[stage]).start()

    send_all(0, sb1, rb1)

    line_id = iota((lines, width), 0)
    first_j = line_id % sy == 0

    def back_j(x, edge):
        edge_full = jnp.broadcast_to(edge, (sx, sy, width)).reshape(lines, width)
        shifted = jnp.concatenate([x[lines - 1 :, :], x[: lines - 1, :]], axis=0)
        return jnp.where(first_j, edge_full, shifted)

    halo[0].wait()
    edge = hy[...]
    sb2[...] = pick(place, back_j(w, edge)).reshape(n, s, width)
    send_all(1, sb2, rb2)

    for copy in halo[1:]:
        copy.wait()
    x1 = jnp.concatenate([hx[...], w[: lines - sy, :]], axis=0)
    x3 = back_j(x1, jnp.concatenate([hc[...].reshape(1, 1, width), edge[: sx - 1]], axis=0))
    for c, x in enumerate((x1, x3)):
        sb3[:, c * s : (c + 1) * s, :] = pick(place, x).reshape(n, s, width)

    lane = iota((1, lines), 1)
    at_j0 = lane % sy == 0
    r0, rx, ry, rxy = hr[0], hr[1], hr[2], hr[3]
    rim1 = jnp.where(lane < sy, roll_lanes(rx, sy), roll_lanes(r0, sy))
    rim2 = jnp.where(at_j0, roll_lanes(ry, 1 - sy), roll_lanes(r0, 1))
    edge_rim = jnp.where(lane == 0, roll_lanes(rxy, 1), roll_lanes(ry, 1))
    rim3 = jnp.where(at_j0, edge_rim, roll_lanes(rim1, 1))
    rims = jnp.where(group == 0, r0, jnp.where(group == 1, rim1, jnp.where(group == 2, rim2, rim3)))
    rims = jnp.where(at_rank & (group < 4), rims, 0.0)
    sb3[:, 2 * s : 2 * s + 1, :] = pick(mine_b, rims, NT).reshape(n, 1, width)

    send_all(2, sb3, rb3)

    pltpu.make_async_copy(rb1, rb1, r_sem.at[0]).wait()
    col_id = iota((width, lines), 1)
    from_dev = iota((n, lines), 1) // s == iota((n, lines), 0)

    def spread(extra, q):
        sel = onehot(row_id == q * s + col_id % s)
        return jnp.sum(jnp.where(from_dev, pick_r(extra, sel), 0.0), axis=0, keepdims=True)

    slot_in = spread(rb1[:, s : s + 1, :].reshape(n, width), 0).astype(I32)
    to_slot = onehot(slot_in == iota((lines, lines), 0))
    cur_ref[0] = pick(to_slot, rb1[:, 0:s, :].reshape(lines, width))

    pltpu.make_async_copy(rb2, rb2, r_sem.at[1]).wait()
    cur_ref[2] = pick(to_slot, rb2[...].reshape(lines, width))

    pltpu.make_async_copy(rb3, rb3, r_sem.at[2]).wait()
    for c in range(2):
        cur_ref[2 * c + 1] = pick(to_slot, rb3[:, c * s : (c + 1) * s, :].reshape(lines, width))
    extra = rb3[:, 2 * s : 2 * s + 1, :].reshape(n, width)
    got = [spread(extra, q) for q in range(4)]
    rows = jnp.zeros((width, lines), F32)
    for q in range(4):
        rows = jnp.where(row_id == q, got[q], rows)
    bef_ref[...] = pick(to_slot, rows, NT)

    for stage, sb in enumerate((sb1, sb2, sb3)):
        sent = sb.at[pl.ds(0, n - 1)]
        pltpu.make_async_copy(sent, sent, s_sem.at[stage]).wait()


def finish(cur_ref, bef_ref, out_ref, lump_ref):
    shape = cur_ref.shape[1:]
    at_0 = iota(shape, 1) == 0
    near, far = [], []
    for c in range(4):
        x = cur_ref[c] * 0.015625
        shifted = pltpu.roll(x, 1, axis=1)
        near.append(x)
        far.append(jnp.where(at_0, bef_ref[:, c : c + 1] * 0.015625, shifted))

    def triple(c, b):
        return (b, 2.0 * (c + b), c)

    def nine(v):
        by_x0 = triple(v[0], v[1])
        by_x1 = triple(v[2], v[3])
        return [triple(by_x0[o1], by_x1[o1]) for o1 in range(3)]

    cur, back = nine(near), nine(far)
    for o1 in range(3):
        for o2 in range(3):
            for o3, value in enumerate(triple(cur[o1][o2], back[o1][o2])):
                out_ref[9 * o1 + 3 * o2 + o3] = value
    total = functools.reduce(lambda a, b: a + b, near + far)
    lump_ref[...] = 1.0 / (27.0 * total)


def shards(sizes, cell_volume, exponent, owner_row):
    sx, sy, width = cell_volume.shape
    lines = sx * sy
    n = sizes[0] * sizes[1] * sizes[2]
    s = lines // n
    vmem = pl.BlockSpec(memory_space=pltpu.VMEM)
    dma = pltpu.SemaphoreType.DMA
    cur, bef = pl.pallas_call(
        functools.partial(exchange, sizes),
        out_shape=(
            jax.ShapeDtypeStruct((4, lines, width), F32),
            jax.ShapeDtypeStruct((lines, width), F32),
        ),
        in_specs=[pl.BlockSpec(memory_space=pltpu.HBM)] * 3,
        out_specs=(vmem, vmem),
        scratch_shapes=[
            pltpu.VMEM((sx, sy, width), F32),
            pltpu.VMEM((sx, sy, width), I32),
            pltpu.VMEM((1, lines), I32),
            dma((3,)),
        ]
        + [pltpu.VMEM((n, rows, width), F32) for rows in (s + 1, s, 2 * s + 1)] * 2
        + [
            pltpu.VMEM((sy, width), F32),
            pltpu.VMEM((sx, 1, width), F32),
            pltpu.VMEM((1, width), F32),
            pltpu.VMEM((1, lines), F32),
            pltpu.VMEM((sy, width), F32),
            pltpu.VMEM((sx, 1, width), F32),
            pltpu.VMEM((1, width), F32),
            pltpu.VMEM((4, 1, lines), F32),
            dma((3,)),
            dma((3,)),
            dma((7,)),
            dma((7,)),
        ],
        compiler_params=pltpu.CompilerParams(
            collective_id=0, has_side_effects=True, vmem_limit_bytes=16 << 20
        ),
    )(cell_volume, exponent, owner_row.reshape(1, lines))
    rows = 64
    return pl.pallas_call(
        finish,
        grid=(lines // rows,),
        out_shape=(
            jax.ShapeDtypeStruct((27, lines, width), F32),
            jax.ShapeDtypeStruct((lines, width), F32),
        ),
        in_specs=[
            pl.BlockSpec((4, rows, width), lambda i: (0, i, 0)),
            pl.BlockSpec((rows, width), lambda i: (i, 0)),
        ],
        out_specs=(
            pl.BlockSpec((27, rows, width), lambda i: (0, i, 0)),
            pl.BlockSpec((rows, width), lambda i: (i, 0)),
        ),
        compiler_params=pltpu.CompilerParams(vmem_limit_bytes=16 << 20),
    )(cur, bef)


def solution(mesh):
    sizes = tuple(mesh.shape[a] for a in AXES)
    return jax.shard_map(
        functools.partial(shards, sizes),
        mesh=mesh,
        in_specs=(P(*AXES), P(*AXES), P(AXES)),
        out_specs=(P(None, AXES, None), P(AXES, None)),
        check_vma=False,
    )
```

```python
import functools

import jax
import jax.numpy as jnp
from jax import lax
from jax.experimental import pallas as pl
from jax.experimental.pallas import tpu as pltpu
from jax.sharding import PartitionSpec as P

MESH = pl.DeviceIdType.MESH
AXES = ("gx", "gy", "gz")
F32, BF16, I32 = jnp.float32, jnp.bfloat16, jnp.int32
log_step = 0.3
NN = (((1,), (0,)), ((), ()))
NT = (((1,), (1,)), ((), ()))


def onehot(mask):
    return jnp.where(mask, 1.0, 0.0).astype(BF16)


def halves(x):
    hi = x.astype(BF16)
    return hi, (x - hi.astype(F32)).astype(BF16)


def pick(sel, x, dims=NN):
    total = None
    for part in halves(x):
        term = lax.dot_general(sel, part, dims, preferred_element_type=F32)
        total = term if total is None else total + term
    return total


def pick_r(x, sel, dims=NN):
    total = None
    for part in halves(x):
        term = lax.dot_general(part, sel, dims, preferred_element_type=F32)
        total = term if total is None else total + term
    return total


def iota(shape, dim):
    return lax.broadcasted_iota(I32, shape, dim)


def roll_lanes(x, shift):
    width = x.shape[1]
    cut = width - shift % width
    return jnp.concatenate([x[:, cut:], x[:, :cut]], axis=1)


def exchange(
    sizes, cv_hbm, ex_hbm, own_hbm, cur_ref, bef_ref,
    cv_ref, ex_ref, own_ref, in_sem,
    sb1, sb2, sb3, rb1, rb2, rb3, tx, ty, tc, tr, hx, hy, hc, hr,
    s_sem, r_sem, hs_sem, hr_sem,
):
    nx, ny, nz = sizes
    n = nx * ny * nz
    gx, gy, gz = (lax.axis_index(a) for a in AXES)
    me = (gx * ny + gy) * nz + gz
    sx, sy, width = cv_ref.shape
    lines = sx * sy
    s = lines // n

    def coords(d):
        return (d // (ny * nz), (d // nz) % ny, d % nz)

    arrive = []
    for i, (src, dst) in enumerate(((own_hbm, own_ref), (cv_hbm, cv_ref), (ex_hbm, ex_ref))):
        copy = pltpu.make_async_copy(src, dst, in_sem.at[i])
        copy.start()
        arrive.append(copy)
    barrier = pltpu.get_barrier_semaphore()

    def greet(k, carry):
        d = (me + k) % n
        pl.semaphore_signal(barrier, inc=1, device_id=coords(d), device_id_type=MESH)
        return carry

    lax.fori_loop(1, n, greet, 0)

    arrive[0].wait()
    owner_full = own_ref[...]
    owner = owner_full // lines
    slot = (owner_full % lines).astype(F32)
    mine = owner == iota((n, lines), 0)
    mine_b = onehot(mine)
    below = onehot(iota((lines, lines), 0) < iota((lines, lines), 1))
    counts = lax.dot_general(mine_b, below, NN, preferred_element_type=F32)
    rank = jnp.sum(jnp.where(mine, counts, 0.0), axis=0, keepdims=True).astype(I32)
    place = onehot(owner * s + rank == iota((lines, lines), 0))

    row_id = iota((width, lines), 0)
    at_rank = rank == row_id % s
    group = row_id // s

    arrive[1].wait()
    arrive[2].wait()
    w3 = cv_ref[...] * jnp.exp(-log_step * ex_ref[...].astype(F32))
    w = w3.reshape(lines, width)
    tx[...] = w[lines - sy :, :]
    ty[...] = w3[:, sy - 1 :, :]
    tc[...] = w[lines - 1 :, :]
    last = onehot(iota((8, width), 1) == width - 1)
    tr[...] = pick(last, w, NT)[0:1, :]

    packed0 = pick(place, w)
    sb1[:, 0:s, :] = packed0.reshape(n, s, width)
    slots = pick(mine_b, jnp.where(at_rank & (group == 0), slot, 0.0), NT)
    sb1[:, s : s + 1, :] = slots.reshape(n, 1, width)

    pl.semaphore_wait(barrier, n - 1)

    ux, uy, uz = (gx + 1) % nx, (gy + 1) % ny, (gz + 1) % nz
    halo = []
    routes = [
        (ty, hy, (gx, uy, gz)),
        (tx, hx, (ux, gy, gz)),
        (tc, hc, (ux, uy, gz)),
        (tr, hr.at[0], (gx, gy, uz)),
        (tr, hr.at[1], (ux, gy, uz)),
        (tr, hr.at[2], (gx, uy, uz)),
        (tr, hr.at[3], (ux, uy, uz)),
    ]
    for i, (src, dst, to) in enumerate(routes):
        copy = pltpu.make_async_remote_copy(
            src_ref=src, dst_ref=dst, send_sem=hs_sem.at[i], recv_sem=hr_sem.at[i],
            device_id=to, device_id_type=MESH,
        )
        copy.start()
        halo.append(copy)

    def send_all(stage, sb, rb):
        def send(k, carry):
            a, r = k // (ny * nz), k % (ny * nz)
            px, py, pz = (gx + a) % nx, (gy + r // nz) % ny, (gz + r % nz) % nz
            d = (px * ny + py) * nz + pz
            pltpu.make_async_remote_copy(
                src_ref=sb.at[d], dst_ref=rb.at[me], send_sem=s_sem.at[stage], recv_sem=r_sem.at[stage],
                device_id=coords(d), device_id_type=MESH,
            ).start()
            return carry

        lax.fori_loop(n // 2, n, send, 0)
        lax.fori_loop(ny * nz, n // 2, send, 0)
        lax.fori_loop(1, ny * nz, send, 0)
        pltpu.make_async_copy(sb.at[me], rb.at[me], r_sem.at[stage]).start()

    send_all(0, sb1, rb1)

    line_id = iota((lines, width), 0)
    first_j = line_id % sy == 0

    def back_j(x, edge):
        edge_full = jnp.broadcast_to(edge, (sx, sy, width)).reshape(lines, width)
        shifted = jnp.concatenate([x[lines - 1 :, :], x[: lines - 1, :]], axis=0)
        return jnp.where(first_j, edge_full, shifted)

    halo[0].wait()
    edge = hy[...]
    sb2[...] = pick(place, back_j(w, edge)).reshape(n, s, width)
    send_all(1, sb2, rb2)

    for copy in halo[1:]:
        copy.wait()
    x1 = jnp.concatenate([hx[...], w[: lines - sy, :]], axis=0)
    x3 = back_j(x1, jnp.concatenate([hc[...].reshape(1, 1, width), edge[: sx - 1]], axis=0))
    for c, x in enumerate((x1, x3)):
        sb3[:, c * s : (c + 1) * s, :] = pick(place, x).reshape(n, s, width)

    lane = iota((1, lines), 1)
    at_j0 = lane % sy == 0
    r0, rx, ry, rxy = hr[0], hr[1], hr[2], hr[3]
    rim1 = jnp.where(lane < sy, roll_lanes(rx, sy), roll_lanes(r0, sy))
    rim2 = jnp.where(at_j0, roll_lanes(ry, 1 - sy), roll_lanes(r0, 1))
    edge_rim = jnp.where(lane == 0, roll_lanes(rxy, 1), roll_lanes(ry, 1))
    rim3 = jnp.where(at_j0, edge_rim, roll_lanes(rim1, 1))
    rims = jnp.where(group == 0, r0, jnp.where(group == 1, rim1, jnp.where(group == 2, rim2, rim3)))
    rims = jnp.where(at_rank & (group < 4), rims, 0.0)
    sb3[:, 2 * s : 2 * s + 1, :] = pick(mine_b, rims, NT).reshape(n, 1, width)

    send_all(2, sb3, rb3)

    pltpu.make_async_copy(rb1, rb1, r_sem.at[0]).wait()
    col_id = iota((width, lines), 1)
    from_dev = iota((n, lines), 1) // s == iota((n, lines), 0)

    def spread(extra, q):
        sel = onehot(row_id == q * s + col_id % s)
        return jnp.sum(jnp.where(from_dev, pick_r(extra, sel), 0.0), axis=0, keepdims=True)

    slot_in = spread(rb1[:, s : s + 1, :].reshape(n, width), 0).astype(I32)
    to_slot = onehot(slot_in == iota((lines, lines), 0))
    cur_ref[0] = pick(to_slot, rb1[:, 0:s, :].reshape(lines, width))

    pltpu.make_async_copy(rb2, rb2, r_sem.at[1]).wait()
    cur_ref[2] = pick(to_slot, rb2[...].reshape(lines, width))

    pltpu.make_async_copy(rb3, rb3, r_sem.at[2]).wait()
    for c in range(2):
        cur_ref[2 * c + 1] = pick(to_slot, rb3[:, c * s : (c + 1) * s, :].reshape(lines, width))
    extra = rb3[:, 2 * s : 2 * s + 1, :].reshape(n, width)
    got = [spread(extra, q) for q in range(4)]
    rows = jnp.zeros((width, lines), F32)
    for q in range(4):
        rows = jnp.where(row_id == q, got[q], rows)
    bef_ref[...] = pick(to_slot, rows, NT)

    for stage, sb in enumerate((sb1, sb2, sb3)):
        sent = sb.at[pl.ds(0, n - 1)]
        pltpu.make_async_copy(sent, sent, s_sem.at[stage]).wait()


def finish(cur_ref, bef_ref, out_ref, lump_ref):
    shape = cur_ref.shape[1:]
    at_0 = iota(shape, 1) == 0
    near, far = [], []
    for c in range(4):
        x = cur_ref[c] * 0.015625
        shifted = pltpu.roll(x, 1, axis=1)
        near.append(x)
        far.append(jnp.where(at_0, bef_ref[:, c : c + 1] * 0.015625, shifted))

    def triple(c, b):
        return (b, 2.0 * (c + b), c)

    def nine(v):
        by_x0 = triple(v[0], v[1])
        by_x1 = triple(v[2], v[3])
        return [triple(by_x0[o1], by_x1[o1]) for o1 in range(3)]

    cur, back = nine(near), nine(far)
    for o1 in range(3):
        for o2 in range(3):
            for o3, value in enumerate(triple(cur[o1][o2], back[o1][o2])):
                out_ref[9 * o1 + 3 * o2 + o3] = value
    total = functools.reduce(lambda a, b: a + b, near + far)
    lump_ref[...] = 1.0 / (27.0 * total)


def shards(sizes, cell_volume, exponent, owner_row):
    sx, sy, width = cell_volume.shape
    lines = sx * sy
    n = sizes[0] * sizes[1] * sizes[2]
    s = lines // n
    vmem = pl.BlockSpec(memory_space=pltpu.VMEM)
    dma = pltpu.SemaphoreType.DMA
    cur, bef = pl.pallas_call(
        functools.partial(exchange, sizes),
        out_shape=(
            jax.ShapeDtypeStruct((4, lines, width), F32),
            jax.ShapeDtypeStruct((lines, width), F32),
        ),
        in_specs=[pl.BlockSpec(memory_space=pltpu.HBM)] * 3,
        out_specs=(vmem, vmem),
        scratch_shapes=[
            pltpu.VMEM((sx, sy, width), F32),
            pltpu.VMEM((sx, sy, width), I32),
            pltpu.VMEM((1, lines), I32),
            dma((3,)),
        ]
        + [pltpu.VMEM((n, rows, width), F32) for rows in (s + 1, s, 2 * s + 1)] * 2
        + [
            pltpu.VMEM((sy, width), F32),
            pltpu.VMEM((sx, 1, width), F32),
            pltpu.VMEM((1, width), F32),
            pltpu.VMEM((1, lines), F32),
            pltpu.VMEM((sy, width), F32),
            pltpu.VMEM((sx, 1, width), F32),
            pltpu.VMEM((1, width), F32),
            pltpu.VMEM((4, 1, lines), F32),
            dma((3,)),
            dma((3,)),
            dma((7,)),
            dma((7,)),
        ],
        compiler_params=pltpu.CompilerParams(
            collective_id=0, has_side_effects=True, vmem_limit_bytes=16 << 20
        ),
    )(*(pltpu.with_memory_space_constraint(a, pltpu.HBM) for a in (cell_volume, exponent, owner_row.reshape(1, lines))))
    rows = 128
    return pl.pallas_call(
        finish,
        grid=(lines // rows,),
        out_shape=(
            jax.ShapeDtypeStruct((27, lines, width), F32),
            jax.ShapeDtypeStruct((lines, width), F32),
        ),
        in_specs=[
            pl.BlockSpec((4, rows, width), lambda i: (0, i, 0)),
            pl.BlockSpec((rows, width), lambda i: (i, 0)),
        ],
        out_specs=(
            pl.BlockSpec((27, rows, width), lambda i: (0, i, 0)),
            pl.BlockSpec((rows, width), lambda i: (i, 0)),
        ),
        compiler_params=pltpu.CompilerParams(vmem_limit_bytes=16 << 20),
    )(cur, bef)


def solution(mesh):
    sizes = tuple(mesh.shape[a] for a in AXES)
    return jax.shard_map(
        functools.partial(shards, sizes),
        mesh=mesh,
        in_specs=(P(*AXES), P(*AXES), P(AXES)),
        out_specs=(P(None, AXES, None), P(AXES, None)),
        check_vma=False,
    )
```
